32 devices in a mesh: dp: 4 (over y, x), fsdp: 8 (over z, core).
Axes of the slice: x: 2, y: 2, z: 4, core: 2. Of those that a mesh axis runs over, the one named last changes fastest.
Arguments:
- tokens: bfloat16 [32768, 768], P(('dp', 'fsdp')), may hold values from -6 to 6
- segment_ids: int32 [64, 512], P(('dp', 'fsdp')), may hold values from 0 to 7, as said below
- out_grad: bfloat16 [32768, 768], P(('dp', 'fsdp')), may hold values from -6 to 6
- qkv_weight: bfloat16 [768, 2304], P(('dp', 'fsdp')), may hold values from -0.21875 to 0.21875
- query_bias: bfloat16 [768], P(('dp', 'fsdp')), may hold values from -4 to 4
- value_bias: bfloat16 [768], P(('dp', 'fsdp')), may hold values from -4 to 4
- out_weight: bfloat16 [768, 768], P(('dp', 'fsdp')), may hold values from -0.875 to 0.875
- out_bias: bfloat16 [768], P(('dp', 'fsdp')), may hold values from -4 to 4
- attn_gain: bfloat16 [768], P(('dp', 'fsdp')), may hold values from 0.099609375 to 1.8984375
- attn_shift: bfloat16 [768], P(('dp', 'fsdp')), may hold values from -4 to 4
- up_weight: bfloat16 [768, 3072], P(('dp', 'fsdp')), may hold values from -0.21875 to 0.21875
- up_bias: bfloat16 [3072], P(('dp', 'fsdp')), may hold values from -4 to 4
- down_weight: bfloat16 [3072, 768], P(('dp', 'fsdp')), may hold values from -0.109375 to 0.109375
- down_bias: bfloat16 [768], P(('dp', 'fsdp')), may hold values from -4 to 4
- final_gain: bfloat16 [768], P(('dp', 'fsdp')), may hold values from 0.099609375 to 1.8984375
- final_shift: bfloat16 [768], P(('dp', 'fsdp')), may hold values from -4 to 4
Outputs:
- layer_out: bfloat16 [32768, 768], P(('dp', 'fsdp'))
- pooled: float32 [64, 8, 5, 768], P(('dp', 'fsdp'))
- tokens_grad: bfloat16 [32768, 768], P(('dp', 'fsdp'))
- qkv_weight_grad: float32 [768, 2304], P(('dp', 'fsdp'))
- query_bias_grad: float32 [768], P(('dp', 'fsdp'))
- value_bias_grad: float32 [768], P(('dp', 'fsdp'))
- out_weight_grad: float32 [768, 768], P(('dp', 'fsdp'))
- out_bias_grad: float32 [768], P(('dp', 'fsdp'))
- attn_gain_grad: float32 [768], P(('dp', 'fsdp'))
- attn_shift_grad: float32 [768], P(('dp', 'fsdp'))
- up_weight_grad: float32 [768, 3072], P(('dp', 'fsdp'))
- up_bias_grad: float32 [3072], P(('dp', 'fsdp'))
- down_weight_grad: float32 [3072, 768], P(('dp', 'fsdp'))
- down_bias_grad: float32 [768], P(('dp', 'fsdp'))
- final_gain_grad: float32 [768], P(('dp', 'fsdp'))
- final_shift_grad: float32 [768], P(('dp', 'fsdp'))
The draws below stay inside these ranges and needn't reach their ends.
Inputs may be any that keep to these rules, and one draw needn't show every extreme that they name: `segment_ids`: in every packed row ids start at 0, never fall and rise by at most 1, so a row holds 1 to 8 segments; row 0 holds 8.
All inputs are finite; a program needn't handle non-finite values.
Results may differ from the reference program's by a relative error of at most 0.014.
Values may be sent and summed in bfloat16 or wider, within the bound.
A program may use at most 192 MiB of HBM per device.

```python
import jax
import jax.numpy as jnp
from jax import lax

D = 768
HEADS = 12
HD = 64
FF = 3072
LEN = 512
SEGS = 8
NPREF = 5
ROWS = 64
TOKENS = 32768


def draw_segment_ids(key, part):
    cut_key, keep_key = jax.random.split(key)
    row_keys = jax.random.split(cut_key, ROWS)
    places = jax.vmap(lambda row_key: jax.random.permutation(row_key, LEN - 1))(row_keys)[:, :SEGS - 1] + 1
    active = jax.random.randint(keep_key, (ROWS, SEGS - 1), 0, 2)
    leading = (jnp.arange(ROWS) == 0)[:, None]
    active = jnp.where(leading, 1, active)
    position = jnp.arange(LEN)
    passed = (places[:, :, None] <= position[None, None, :]).astype(jnp.int32) * active[:, :, None]
    return jnp.sum(passed, axis=1).astype(jnp.int32)


def with_spikes(drawn, stream_key, source, target, shards_of, factor):
    owner, partner = [(jnp.arange(drawn.shape[dim]) // (drawn.shape[dim] // shards_of)).reshape([-1 if axis == dim else 1 for axis in range(drawn.ndim)]) for dim in (source, target)]
    chosen = jax.random.permutation(stream_key, shards_of)[partner]
    strong = (owner == chosen) | (owner == (partner + shards_of // 2) % shards_of)
    return jnp.where(strong, factor * drawn, drawn)


def block_scale(key, shape, cuts, low, largest):
    def one(dim, parts):
        steps = jax.random.uniform(jax.random.fold_in(jax.random.fold_in(key, 6), dim), (parts,), jnp.float32, low / len(cuts), largest / len(cuts))
        return jnp.repeat(jnp.exp(steps), shape[dim] // parts).reshape((-1,) + (1,) * (len(shape) - dim - 1))

    level = one(*cuts[0])
    for cut in cuts[1:]:
        level = level * one(*cut)
    return level


def gaussian(key, shape, width, bound, pieces=(), held_as=jnp.bfloat16):
    array = width * jax.random.normal(key, shape, jnp.float32)
    if pieces:
        array = array * block_scale(key, shape, pieces, -0.22, 0.18)
    return jnp.clip(array, -bound, bound).astype(held_as)


def heavy_noise(own_key, dims, scale, most, pieces, heavy, held_as=jnp.bfloat16):
    values = scale * jax.random.normal(own_key, dims, jnp.float32)
    if pieces:
        values = values * block_scale(own_key, dims, pieces, -0.22, 0.18)
    return jnp.clip(with_spikes(values, jax.random.fold_in(own_key, 3), *heavy), -most, most).astype(held_as)


def setup_inputs(seed: int = 0) -> dict:
    streams_of = jax.random.split(jax.random.key(seed), 17)
    return {
        "tokens": heavy_noise(streams_of[0], (TOKENS, D), 1.0, 6.0, ((0, 32),), (0, 1, 32, 2.75)),
        "segment_ids": draw_segment_ids(jax.random.fold_in(streams_of[16], 71), 0),
        "out_grad": gaussian(streams_of[2], (TOKENS, D), 1.0, 6.0, ((0, 32),)),
        "qkv_weight": gaussian(streams_of[3], (D, 3 * D), D ** -0.5, 0.21875, ((0, 32),)),
        "query_bias": gaussian(streams_of[4], (D,), 0.3, 4.0, ((0, 32),)),
        "value_bias": gaussian(streams_of[5], (D,), 0.3, 4.0, ((0, 32),)),
        "out_weight": gaussian(streams_of[6], (D, D), (D // 16) ** -0.5, 0.875, ((0, 32),)),
        "out_bias": gaussian(streams_of[7], (D,), 0.3, 4.0, ((0, 32),)),
        "attn_gain": jnp.clip(1.0 + 0.18 * jax.random.normal(streams_of[8], (D,), jnp.float32), 0.099609375, 1.8984375).astype(jnp.bfloat16),
        "attn_shift": gaussian(streams_of[9], (D,), 0.3, 4.0, ((0, 32),)),
        "up_weight": gaussian(streams_of[10], (D, FF), D ** -0.5, 0.21875, ((0, 32),)),
        "up_bias": gaussian(streams_of[11], (FF,), 0.3, 4.0, ((0, 32),)),
        "down_weight": gaussian(streams_of[12], (FF, D), FF ** -0.5, 0.109375, ((0, 32),)),
        "down_bias": gaussian(streams_of[13], (D,), 0.3, 4.0, ((0, 32),)),
        "final_gain": jnp.clip(1.0 + 0.18 * jax.random.normal(streams_of[14], (D,), jnp.float32), 0.099609375, 1.8984375).astype(jnp.bfloat16),
        "final_shift": gaussian(streams_of[15], (D,), 0.3, 4.0, ((0, 32),)),
    }


@jax.custom_vjp
def low(v):
    return lax.optimization_barrier(v.astype(jnp.bfloat16)).astype(jnp.float32)

@jax.custom_vjp
def low_back(v):
    return v

def low_keep(v):
    return (low(v), None)

def low_pass(kept, grad):
    return (grad,)

def back_keep(v):
    return (v, None)

def back_low(kept, grad):
    return (low(grad),)
low.defvjp(low_keep, low_pass)
low_back.defvjp(back_keep, back_low)

def matmul_high(left, right):
    return jnp.dot(left, right, precision=lax.Precision.HIGHEST)

def layer_norm(values, norm_gain, norm_shift):
    row_mean = lax.optimization_barrier(jnp.mean(values, axis=-1, keepdims=True))
    centered = values - row_mean
    row_var = lax.optimization_barrier(jnp.mean(centered * centered, axis=-1, keepdims=True))
    return centered * lax.rsqrt(row_var + 1e-05) * norm_gain + norm_shift

def attend_row(packed):
    qkv_row, segment_row = packed
    split_row = qkv_row.reshape(LEN, 3, HEADS, HD)
    queries = split_row[:, 0]
    key_part = split_row[:, 1]
    value_part = split_row[:, 2]
    scores = jnp.einsum('qhd,khd->hqk', queries, key_part, precision=lax.Precision.HIGHEST) * HD ** (-0.5)
    scores = low_back(scores)
    allowed = segment_row[:, None] == segment_row[None, :]
    masked = jnp.where(allowed[None], scores, -1000000000.0)
    row_top = lax.optimization_barrier(jnp.max(masked, axis=-1, keepdims=True))
    lifted = jnp.exp(masked - row_top)
    attn_probs = low(lifted / lax.optimization_barrier(jnp.sum(lifted, axis=-1, keepdims=True)))
    context = jnp.einsum('hqk,khd->qhd', attn_probs, value_part, precision=lax.Precision.HIGHEST)
    return context.reshape(LEN, HEADS * HD)

def forward(params, tokens_in, segments):
    qkv_weight, query_bias, value_bias, out_weight, out_bias, attn_gain, attn_shift, up_weight, up_bias, down_weight, down_bias, final_gain, final_shift = params
    qkv_bias = jnp.concatenate([query_bias, jnp.zeros_like(query_bias), value_bias])
    qkv = low(low_back(matmul_high(tokens_in, qkv_weight) + qkv_bias))
    row_count = segments.shape[0]
    context = lax.map(jax.checkpoint(attend_row), (qkv.reshape(row_count, LEN, 3 * D), segments))
    context = low(low_back(context.reshape(row_count * LEN, D)))
    attn_out = low_back(matmul_high(context, out_weight) + out_bias)
    normed = layer_norm(tokens_in + attn_out, attn_gain, attn_shift)
    hidden_pre = low_back(matmul_high(low(normed), up_weight) + up_bias)
    activated = low(jax.nn.gelu(hidden_pre, approximate=False))
    ffn_out = low_back(matmul_high(activated, down_weight) + down_bias)
    return layer_norm(normed + ffn_out, final_gain, final_shift)

def pool_rows(outputs, segment_block):
    row_count = segment_block.shape[0]
    by_row = outputs.reshape(row_count, LEN, D)
    member = (segment_block[:, None, :] == jnp.arange(SEGS)[None, :, None]).astype(jnp.float32)
    seg_sums = jnp.einsum('gsl,gld->gsd', member, by_row, precision=lax.Precision.HIGHEST)
    seg_counts = lax.optimization_barrier(jnp.sum(member, axis=-1, keepdims=True))
    seg_means = seg_sums / jnp.maximum(seg_counts, 1.0)
    columns = jnp.arange(D)
    prefixes = []
    for level in range(NPREF):
        limit = D if level == NPREF - 1 else min(64 * 2 ** level, D)
        kept_cols = seg_means * (columns < limit).astype(jnp.float32)
        prefixes.append(kept_cols * lax.rsqrt(lax.optimization_barrier(jnp.sum(kept_cols * kept_cols, axis=-1, keepdims=True)) + 1e-06))
    return jnp.stack(prefixes, axis=2)

def reference(tokens, segment_ids, out_grad, qkv_weight, query_bias, value_bias, out_weight, out_bias, attn_gain, attn_shift, up_weight, up_bias, down_weight, down_bias, final_gain, final_shift):
    params = tuple((param_in.astype(jnp.float32) for param_in in (qkv_weight, query_bias, value_bias, out_weight, out_bias, attn_gain, attn_shift, up_weight, up_bias, down_weight, down_bias, final_gain, final_shift)))
    rows_total = segment_ids.shape[0]
    per_step = max((candidate for candidate in range(1, rows_total + 1) if rows_total % candidate == 0 and candidate * LEN <= max(4096, LEN)))
    steps_count = rows_total // per_step
    token_blocks = tokens.reshape(steps_count, per_step * LEN, D)
    segment_blocks = segment_ids.reshape(steps_count, per_step, LEN)
    grad_blocks = out_grad.reshape(steps_count, per_step * LEN, D)

    def step_fn(running, block_in):
        token_block, segment_block, grad_block = block_in

        def whole_layer(weights, inputs):
            outputs = forward(weights, inputs, segment_block)
            return (outputs, pool_rows(outputs, segment_block))
        (outputs, pooled_block), pullback = jax.vjp(whole_layer, params, token_block.astype(jnp.float32))
        weight_grads, input_grad = pullback((grad_block.astype(jnp.float32), jnp.zeros_like(pooled_block)))
        running = jax.tree.map(lambda acc_sum, new_term: acc_sum + new_term, running, weight_grads)
        return (running, (outputs.astype(jnp.bfloat16), pooled_block, input_grad.astype(jnp.bfloat16)))
    initial = tuple((jnp.zeros_like(param_in) for param_in in params))
    weight_grads, (layer_blocks, pooled_blocks, input_blocks) = lax.scan(step_fn, initial, (token_blocks, segment_blocks, grad_blocks))
    layer_out = layer_blocks.reshape(rows_total * LEN, D)
    pooled = pooled_blocks.reshape(rows_total, SEGS, NPREF, D)
    tokens_grad = input_blocks.reshape(rows_total * LEN, D)
    return (layer_out, pooled, tokens_grad, weight_grads[0], weight_grads[1], weight_grads[2], weight_grads[3], weight_grads[4], weight_grads[5], weight_grads[6], weight_grads[7], weight_grads[8], weight_grads[9], weight_grads[10], weight_grads[11], weight_grads[12])
```

```python
import functools

import jax
import jax.numpy as jnp
from jax import lax
from jax.experimental import pallas as pl
from jax.experimental.pallas import tpu as pltpu
from jax.sharding import PartitionSpec as P

MESH = pl.DeviceIdType.MESH
BF = jnp.bfloat16
F32 = jnp.float32

def place():
    dp = lax.axis_index("dp")
    fs = lax.axis_index("fsdp")
    return dp, dp // 2, dp % 2, fs // 2, fs % 2


def barrier_all(peers):
    sem = pltpu.get_barrier_semaphore()
    for peer in peers:
        pl.semaphore_signal(sem, inc=1, device_id=peer, device_id_type=MESH)
    pl.semaphore_wait(sem, len(peers))


class Gather:
    SLOTS = 31

    def __init__(self, srcs, outs, send, recv, local):
        self.srcs, self.outs, self.send, self.recv, self.local = srcs, outs, send, recv, local
        dp, y, x, z, c = place()
        self.dp, self.z, self.c = dp, z, c
        self.dpx = y * 2 + (1 - x)
        self.dpy = (1 - y) * 2 + x
        self.dpd = (1 - y) * 2 + (1 - x)
        self.me = self.fs(z)

    def fs(self, z):
        return z * 2 + self.c

    def zk(self, k):
        return (self.z + 4 - k) % 4

    def peers(self):
        return [(self.dp, self.fs((self.z + k) % 4)) for k in (1, 2, 3)] + [
            (self.dpx, self.me), (self.dpy, self.me), (self.dp, self.z * 2 + 1 - self.c)]

    def copy(self, g, dp, z, slot, peer, own=False, n=None):
        index = dp * 8 + self.fs(z)
        src = self.srcs[g] if own else self.outs[g].at[index]
        return pltpu.make_async_remote_copy(
            src_ref=src, dst_ref=self.outs[g].at[index], send_sem=self.send.at[g, slot],
            recv_sem=self.recv.at[g, slot], device_id=peer, device_id_type=MESH)

    def msgs(self, g):
        x, y, core = (self.dpx, self.me), (self.dpy, self.me), (self.dp, self.z * 2 + 1 - self.c)
        out = {}
        for k in (1, 2, 3):
            out[k - 1] = (self.dp, self.z, (self.dp, self.fs((self.z + k) % 4)), True)
        for k in range(4):
            out[3 + k] = (self.dp, self.zk(k), x, k == 0)
            out[7 + k] = (self.dp, self.zk(k), y, k == 0)
            if k < 2:
                out[11 + k] = (self.dpy, self.zk(k), x, False)
            else:
                out[11 + k] = (self.dpx, self.zk(k), y, False)
            out[15 + k] = (self.dp, self.zk(k), core, k == 0)
            out[19 + k] = (self.dpx, self.zk(k), core, False)
            out[23 + k] = (self.dpy, self.zk(k), core, False)
            out[27 + k] = (self.dpd, self.zk(k), core, False)
        return out

    def go(self, g, slot):
        dp, z, peer, own = self.msgs(g)[slot]
        self.copy(g, dp, z, slot, peer, own).start()

    def arrived(self, g, slot):
        dp, z, peer, own = self.msgs(g)[slot]
        self.copy(g, dp, z, slot, peer, own).wait_recv()

    def start(self, g):
        pltpu.make_async_copy(self.srcs[g], self.outs[g].at[self.dp * 8 + self.me], self.local.at[g]).start()
        for slot in (0, 1, 2, 3, 7, 15):
            self.go(g, slot)

    def step_z(self, g, k):
        self.arrived(g, k - 1)
        for slot in (3 + k, 7 + k, 15 + k):
            self.go(g, slot)

    def step_xy(self, g, k):
        self.arrived(g, 3 + k)
        if k >= 2:
            self.go(g, 11 + k)
        self.go(g, 19 + k)
        self.arrived(g, 7 + k)
        if k < 2:
            self.go(g, 11 + k)
        self.go(g, 23 + k)

    def step_d(self, g, k):
        self.arrived(g, 11 + k)
        self.go(g, 27 + k)

    def step_core(self, g):
        for slot in range(15, 31):
            self.arrived(g, slot)

    def drain(self, g):
        pltpu.make_async_copy(self.srcs[g], self.outs[g].at[self.dp * 8 + self.me], self.local.at[g]).wait()
        for slot, (dp, z, peer, own) in self.msgs(g).items():
            self.copy(g, dp, z, slot, peer, own).wait_send()


def gather_kernel(count, *refs):
    srcs, outs = refs[:count], refs[count:2 * count]
    send, recv, local = refs[2 * count:]
    ag = Gather(srcs, outs, send, recv, local)
    barrier_all(ag.peers())
    for g in range(count):
        ag.start(g)
    for k in (1, 2, 3):
        for g in range(count):
            ag.step_z(g, k)
    for k in range(4):
        for g in range(count):
            ag.step_xy(g, k)
    for k in range(4):
        for g in range(count):
            ag.step_d(g, k)
    for g in range(count):
        ag.step_core(g)
    for g in range(count):
        ag.drain(g)


def gather(arrays, cid=0):
    count = len(arrays)
    return pl.pallas_call(
        functools.partial(gather_kernel, count),
        out_shape=[jax.ShapeDtypeStruct((32,) + a.shape, a.dtype) for a in arrays],
        in_specs=[pl.BlockSpec(memory_space=pltpu.VMEM)] * count,
        out_specs=[pl.BlockSpec(memory_space=pl.ANY)] * count,
        scratch_shapes=[pltpu.SemaphoreType.DMA((count, 31)), pltpu.SemaphoreType.DMA((count, 31)),
                        pltpu.SemaphoreType.DMA((count,))],
        compiler_params=pltpu.CompilerParams(collective_id=cid, has_side_effects=True),
    )(*arrays)


class Scatter:
    SLOTS = 31

    def __init__(self, grads, outs, rc, rd, rxy, rz, sb, keep, send, recv):
        self.grads, self.outs = grads, outs
        self.rc, self.rd, self.rxy, self.rz, self.sb, self.keep = rc, rd, rxy, rz, sb, keep
        self.send, self.recv = send, recv
        dp, y, x, z, c = place()
        self.dp, self.z, self.c = dp, z, c
        self.cols = (dp, y * 2 + (1 - x), (1 - y) * 2 + x, (1 - y) * 2 + (1 - x))
        self.me = z * 2 + c

    def zk(self, k):
        return (self.z + 4 - k) % 4

    def peers(self):
        return [(self.dp, self.zk(k) * 2 + self.c) for k in (1, 2, 3)] + [
            (self.cols[1], self.me), (self.cols[2], self.me), (self.dp, self.z * 2 + 1 - self.c)]

    def copy(self, g, slot):
        if slot < 16:
            p, k = divmod(slot, 4)
            index = self.cols[p] * 8 + self.zk(k) * 2 + 1 - self.c
            src, dst, peer = self.grads[g].at[index], self.rc[g].at[slot], (self.dp, self.z * 2 + 1 - self.c)
        elif slot < 20:
            k = slot - 16
            src, dst = self.sb[g].at[12 + k], self.rd[g].at[k]
            peer = (self.cols[1 if k < 2 else 2], self.me)
        elif slot < 28:
            src, dst = self.sb[g].at[slot - 16], self.rxy[g].at[slot - 20]
            peer = (self.cols[1 if slot < 24 else 2], self.me)
        else:
            k = slot - 27
            src, dst, peer = self.sb[g].at[k], self.rz[g].at[k - 1], (self.dp, self.zk(k) * 2 + self.c)
        return pltpu.make_async_remote_copy(
            src_ref=src, dst_ref=dst, send_sem=self.send.at[g, slot], recv_sem=self.recv.at[g, slot],
            device_id=peer, device_id_type=MESH)

    def start(self, g):
        for slot in range(12, 16):
            self.copy(g, slot).start()
        for slot in range(4, 12):
            self.copy(g, slot).start()
        for slot in range(0, 4):
            self.copy(g, slot).start()

    def add(self, g, slot, terms, dst, dtype):
        p, k = divmod(slot, 4)
        index = self.cols[p] * 8 + self.zk(k) * 2 + self.c
        rows, cols = self.grads[g].shape[1:]
        step = 32 if rows % 32 == 0 else rows
        wide = min(cols, 768)

        def part(i, carry):
            at = (pl.ds(0, rows), pl.ds(pl.multiple_of(i * wide, 128), wide)) if step == rows else (
                pl.ds(pl.multiple_of(i * step, step), step), pl.ds(0, cols))
            total = self.grads[g][(index,) + at].astype(F32)
            for ref, j in terms:
                total += ref[(j,) + at].astype(F32)
            if dst is self.outs[g]:
                dst[at] = total
            elif dst is self.keep[g]:
                dst[at] = total
            else:
                dst[(slot,) + at] = total.astype(dtype)
            return carry

        lax.fori_loop(0, cols // wide if step == rows else rows // step, part, 0)

    def step_d(self, g, k):
        self.copy(g, 12 + k).wait_recv()
        self.add(g, 12 + k, [(self.rc[g], 12 + k)], self.sb[g], self.sb[g].dtype)
        self.copy(g, 16 + k).start()

    def step_near(self, g, p, k):
        slot = p * 4 + k
        self.copy(g, slot).wait_recv()
        terms = [(self.rc[g], slot)]
        if (p == 2) == (k < 2):
            self.copy(g, 16 + k).wait_recv()
            terms.append((self.rd[g], k))
        self.add(g, slot, terms, self.sb[g], self.sb[g].dtype)
        self.copy(g, 16 + slot).start()

    def step_own(self, g, k):
        for slot in (k, 20 + k, 24 + k):
            self.copy(g, slot).wait_recv()
        terms = [(self.rc[g], k), (self.rxy[g], k), (self.rxy[g], 4 + k)]
        if k:
            self.add(g, k, terms, self.sb[g], self.sb[g].dtype)
            self.copy(g, 27 + k).start()
        else:
            self.add(g, k, terms, self.keep[g], F32)

    def finish(self, g):
        for slot in (28, 29, 30):
            self.copy(g, slot).wait_recv()
        rows, cols = self.grads[g].shape[1:]
        step = 32 if rows % 32 == 0 else rows
        wide = min(cols, 768)

        def part(i, carry):
            at = (pl.ds(0, rows), pl.ds(pl.multiple_of(i * wide, 128), wide)) if step == rows else (
                pl.ds(pl.multiple_of(i * step, step), step), pl.ds(0, cols))
            total = self.keep[g][at]
            for k in range(3):
                total += self.rz[g][(k,) + at].astype(F32)
            self.outs[g][at] = total
            return carry

        lax.fori_loop(0, cols // wide if step == rows else rows // step, part, 0)

    def drain(self, g):
        for slot in range(31):
            self.copy(g, slot).wait_send()


def scatter_scratch(shapes):
    def bufs(n):
        return [pltpu.VMEM((n, r, c), t) for (r, c, t) in shapes]
    return bufs(16) + bufs(4) + bufs(8) + bufs(3) + bufs(12 + 4) + [pltpu.VMEM((r, c), F32) for (r, c, t) in shapes] + [
        pltpu.SemaphoreType.DMA((len(shapes), 31)), pltpu.SemaphoreType.DMA((len(shapes), 31))]


def scatter_kernel(count, *refs):
    groups = [refs[i * count:(i + 1) * count] for i in range(8)]
    send, recv = refs[8 * count:]
    rs = Scatter(*groups, send, recv)
    barrier_all(rs.peers())
    for g in range(count):
        rs.start(g)
    for k in range(4):
        for g in range(count):
            rs.step_d(g, k)
    for p, k in ((1, 0), (1, 1), (2, 2), (2, 3), (2, 0), (2, 1), (1, 2), (1, 3)):
        for g in range(count):
            rs.step_near(g, p, k)
    for k in (1, 2, 3, 0):
        for g in range(count):
            rs.step_own(g, k)
    for g in range(count):
        rs.finish(g)
    for g in range(count):
        rs.drain(g)


def scatter(arrays, cid=1):
    count = len(arrays)
    shapes = [a.shape[1:] + (a.dtype,) for a in arrays]
    return pl.pallas_call(
        functools.partial(scatter_kernel, count),
        out_shape=[jax.ShapeDtypeStruct(a.shape[1:], F32) for a in arrays],
        in_specs=[pl.BlockSpec(memory_space=pltpu.VMEM)] * count,
        out_specs=[pl.BlockSpec(memory_space=pltpu.VMEM)] * count,
        scratch_shapes=scatter_scratch(shapes),
        compiler_params=pltpu.CompilerParams(collective_id=cid, has_side_effects=True, vmem_limit_bytes=60 * 2**20),
    )(*arrays)


D = 768
HEADS = 12
HD = 64
SEGS = 8
NPREF = 5


def layer_norm(values, norm_gain, norm_shift):
    row_mean = jnp.mean(values, axis=-1, keepdims=True)
    centered = values - row_mean
    row_var = jnp.mean(centered * centered, axis=-1, keepdims=True)
    return centered * lax.rsqrt(row_var + 1e-05) * norm_gain + norm_shift


def gelu_exact(values):
    return jax.nn.gelu(values, approximate=False)


def divisor_below(count, limit):
    return max(
        (
            candidate
            for candidate in range(1, count + 1)
            if count % candidate == 0 and candidate <= limit
        )
    )


def masked_scores(queries, key_part, segment_group):
    scores = jnp.einsum(
        "gqhd,gkhd->ghqk", queries, key_part, preferred_element_type=jnp.float32
    ) * HD ** (-0.5)
    allowed = (segment_group[:, :, None] == segment_group[:, None, :])[:, None]
    return jnp.where(allowed, scores, -1000000000.0)


def attend_forward(packed):
    qkv_group, segment_group = packed
    masked = masked_scores(qkv_group[:, :, 0], qkv_group[:, :, 1], segment_group)
    row_top = jnp.max(masked, axis=-1, keepdims=True)
    lifted = jnp.exp(masked - row_top)
    row_total = jnp.sum(lifted, axis=-1, keepdims=True)
    attn_probs = lifted / row_total
    context = jnp.einsum(
        "ghqk,gkhd->gqhd",
        attn_probs.astype(jnp.bfloat16),
        qkv_group[:, :, 2],
        preferred_element_type=jnp.float32,
    ).astype(jnp.bfloat16)
    return (context, row_top + jnp.log(row_total))


def attend_backward(packed):
    qkv_group, segment_group, grad_group, log_total = packed
    queries = qkv_group[:, :, 0]
    key_part = qkv_group[:, :, 1]
    value_part = qkv_group[:, :, 2]
    attn_probs = jnp.exp(masked_scores(queries, key_part, segment_group) - log_total)
    prob_grad = jnp.einsum(
        "gqhd,gkhd->ghqk", grad_group, value_part, preferred_element_type=jnp.float32
    )
    row_dot = jnp.sum(attn_probs * prob_grad, axis=-1, keepdims=True)
    score_grad = (attn_probs * (prob_grad - row_dot)).astype(jnp.bfloat16)
    value_grad = jnp.einsum(
        "ghqk,gqhd->gkhd",
        attn_probs.astype(jnp.bfloat16),
        grad_group,
        preferred_element_type=jnp.float32,
    )
    query_grad = jnp.einsum(
        "ghqk,gkhd->gqhd", score_grad, key_part, preferred_element_type=jnp.float32
    ) * HD ** (-0.5)
    key_grad = jnp.einsum(
        "ghqk,gqhd->gkhd", score_grad, queries, preferred_element_type=jnp.float32
    ) * HD ** (-0.5)
    return jnp.stack([query_grad, key_grad, value_grad], axis=2).astype(jnp.bfloat16)


def pool_rows(outputs, segment_block):
    row_count = segment_block.shape[0]
    length = segment_block.shape[1]
    by_row = outputs.reshape(row_count, length, D)
    member = (segment_block[:, None, :] == jnp.arange(SEGS)[None, :, None]).astype(jnp.float32)
    seg_sums = jnp.einsum("gsl,gld->gsd", member, by_row, precision=lax.Precision.HIGHEST)
    seg_counts = jnp.sum(member, axis=-1, keepdims=True)
    seg_means = seg_sums / jnp.maximum(seg_counts, 1.0)
    columns = jnp.arange(D)
    prefixes = []
    for level in range(NPREF):
        limit = D if level == NPREF - 1 else min(64 * 2**level, D)
        kept_cols = seg_means * (columns < limit).astype(jnp.float32)
        prefixes.append(
            kept_cols * lax.rsqrt(jnp.sum(kept_cols * kept_cols, axis=-1, keepdims=True) + 1e-06)
        )
    return jnp.stack(prefixes, axis=2)

AXES = ("dp", "fsdp")


def gather_all(kernels, weights, vectors, wide):
    if not kernels:
        return [lax.all_gather(a, AXES, axis=0, tiled=True) for a in (*weights, *vectors, wide)]
    part = vectors[0].shape[0]
    small = jnp.concatenate([*vectors, wide])
    small = jnp.pad(small, (0, 2048 - small.shape[0])).reshape(16, 128)
    outs = gather((*weights, small))
    full = [a.reshape(-1, a.shape[-1]) for a in outs[:-1]]
    flat = outs[-1].reshape(32, 2048)
    rows = flat[:, :len(vectors) * part].reshape(32, len(vectors), part).transpose(1, 0, 2).reshape(len(vectors), -1)
    wide_full = flat[:, len(vectors) * part:len(vectors) * part + wide.shape[0]].reshape(-1)
    return [*full, *rows, wide_full]


def scatter_all(kernels, grads, vectors, wide):
    if not kernels:
        return [lax.psum_scatter(a.astype(F32), AXES, scatter_dimension=0, tiled=True) for a in (*grads, *vectors, wide)]
    part = vectors[0].shape[0] // 32
    small = jnp.stack(vectors).reshape(len(vectors), 32, part).transpose(1, 0, 2).reshape(32, -1)
    small = jnp.concatenate([small, wide.reshape(32, -1)], axis=1)
    small = jnp.pad(small, ((0, 0), (0, 1024 - small.shape[1]))).reshape(32, 8, 128)
    outs = scatter([a.astype(BF).reshape(32, -1, a.shape[-1]) for a in grads] + [small])
    flat = outs[-1].reshape(-1)
    n = len(vectors) * part
    return [*outs[:-1], *[flat[i * part:(i + 1) * part] for i in range(len(vectors))], flat[n:n + wide.shape[0] // 32]]


def per_device(
    kernels,
    tokens,
    segment_ids,
    out_grad,
    qkv_weight,
    query_bias,
    value_bias,
    out_weight,
    out_bias,
    attn_gain,
    attn_shift,
    up_weight,
    up_bias,
    down_weight,
    down_bias,
    final_gain,
    final_shift,
):
    (qkv_full, out_full, up_full, down_full, query_full, value_full, out_bias_full, attn_gain_full,
     attn_shift_full, down_bias_full, final_gain_full, final_shift_full, up_bias_full) = gather_all(
        kernels, (qkv_weight, out_weight, up_weight, down_weight),
        (query_bias, value_bias, out_bias, attn_gain, attn_shift, down_bias, final_gain, final_shift), up_bias)
    width = out_full.shape[0]
    row_count, length = segment_ids.shape
    per_group = divisor_below(row_count, max(1, 512 // length))
    groups = row_count // per_group
    qkv_bias = jnp.concatenate([query_full, jnp.zeros_like(query_full), value_full]).astype(
        jnp.float32
    )
    qkv = (jnp.dot(tokens, qkv_full, preferred_element_type=jnp.float32) + qkv_bias).astype(
        jnp.bfloat16
    )
    qkv_groups = qkv.reshape(groups, per_group, length, 3, HEADS, HD)
    segment_groups = segment_ids.reshape(groups, per_group, length)
    context, log_total = lax.map(attend_forward, (qkv_groups, segment_groups))
    context = context.reshape(row_count * length, width)
    attn_out = jnp.dot(
        context, out_full, preferred_element_type=jnp.float32
    ) + out_bias_full.astype(jnp.float32)
    resid_one = tokens.astype(jnp.float32) + attn_out
    normed = layer_norm(
        resid_one, attn_gain_full.astype(jnp.float32), attn_shift_full.astype(jnp.float32)
    )
    normed_low = normed.astype(jnp.bfloat16)
    hidden_pre = jnp.dot(
        normed_low, up_full, preferred_element_type=jnp.float32
    ) + up_bias_full.astype(jnp.float32)
    activated = gelu_exact(hidden_pre).astype(jnp.bfloat16)
    ffn_out = jnp.dot(
        activated, down_full, preferred_element_type=jnp.float32
    ) + down_bias_full.astype(jnp.float32)
    resid_two = normed + ffn_out
    final_out, final_pull = jax.vjp(
        layer_norm,
        resid_two,
        final_gain_full.astype(jnp.float32),
        final_shift_full.astype(jnp.float32),
    )
    pooled = pool_rows(final_out, segment_ids)
    resid_two_grad, final_gain_grad, final_shift_grad = final_pull(out_grad.astype(jnp.float32))
    ffn_grad = resid_two_grad.astype(jnp.bfloat16)
    down_weight_grad = jnp.einsum(
        "tf,td->fd", activated, ffn_grad, preferred_element_type=jnp.float32
    )
    down_bias_grad = jnp.sum(ffn_grad.astype(jnp.float32), axis=0)
    act_grad = jnp.einsum("td,fd->tf", ffn_grad, down_full, preferred_element_type=jnp.float32)
    _, gelu_pull = jax.vjp(gelu_exact, hidden_pre)
    hidden_grad = gelu_pull(act_grad)[0].astype(jnp.bfloat16)
    up_weight_grad = jnp.einsum(
        "td,tf->df", normed_low, hidden_grad, preferred_element_type=jnp.float32
    )
    up_bias_grad = jnp.sum(hidden_grad.astype(jnp.float32), axis=0)
    normed_grad = resid_two_grad + jnp.einsum(
        "tf,df->td", hidden_grad, up_full, preferred_element_type=jnp.float32
    )
    _, attn_pull = jax.vjp(
        layer_norm, resid_one, attn_gain_full.astype(jnp.float32), attn_shift_full.astype(jnp.float32)
    )
    resid_one_grad, attn_gain_grad, attn_shift_grad = attn_pull(normed_grad)
    attn_grad = resid_one_grad.astype(jnp.bfloat16)
    out_weight_grad = jnp.einsum(
        "td,te->de", context, attn_grad, preferred_element_type=jnp.float32
    )
    out_bias_grad = jnp.sum(attn_grad.astype(jnp.float32), axis=0)
    context_grad = jnp.einsum(
        "te,de->td", attn_grad, out_full, preferred_element_type=jnp.float32
    ).astype(jnp.bfloat16)
    grad_groups = context_grad.reshape(groups, per_group, length, HEADS, HD)
    qkv_grad = lax.map(attend_backward, (qkv_groups, segment_groups, grad_groups, log_total))
    qkv_grad = qkv_grad.reshape(row_count * length, 3 * width)
    qkv_weight_grad = jnp.einsum("td,te->de", tokens, qkv_grad, preferred_element_type=jnp.float32)
    query_bias_grad = jnp.sum(qkv_grad[:, :width].astype(jnp.float32), axis=0)
    value_bias_grad = jnp.sum(qkv_grad[:, 2 * width :].astype(jnp.float32), axis=0)
    tokens_grad = (
        resid_one_grad
        + jnp.einsum("te,de->td", qkv_grad, qkv_full, preferred_element_type=jnp.float32)
    ).astype(jnp.bfloat16)
    sums = scatter_all(
        kernels, (qkv_weight_grad, out_weight_grad, up_weight_grad, down_weight_grad),
        (query_bias_grad, value_bias_grad, out_bias_grad, attn_gain_grad, attn_shift_grad, down_bias_grad,
         final_gain_grad, final_shift_grad), up_bias_grad)
    gq, go, gu, gd, gqb, gvb, gob, gag, gas, gdb, gfg, gfs, gub = sums
    return (
        final_out.astype(jnp.bfloat16), pooled, tokens_grad,
        gq, gqb, gvb, go, gob, gag, gas, gu, gub, gd, gdb, gfg, gfs,
    )


def solution(mesh):
    kernels = dict(mesh.shape) == {"dp": 4, "fsdp": 8}
    return jax.shard_map(
        functools.partial(per_device, kernels),
        mesh=mesh,
        in_specs=(
            P(("dp", "fsdp"), None),
            P(("dp", "fsdp"), None),
            P(("dp", "fsdp"), None),
            P(("dp", "fsdp"), None),
            P(("dp", "fsdp")),
            P(("dp", "fsdp")),
            P(("dp", "fsdp"), None),
            P(("dp", "fsdp")),
            P(("dp", "fsdp")),
            P(("dp", "fsdp")),
            P(("dp", "fsdp"), None),
            P(("dp", "fsdp")),
            P(("dp", "fsdp"), None),
            P(("dp", "fsdp")),
            P(("dp", "fsdp")),
            P(("dp", "fsdp")),
        ),
        out_specs=(
            P(("dp", "fsdp"), None),
            P(("dp", "fsdp"), None, None, None),
            P(("dp", "fsdp"), None),
            P(("dp", "fsdp"), None),
            P(("dp", "fsdp")),
            P(("dp", "fsdp")),
            P(("dp", "fsdp"), None),
            P(("dp", "fsdp")),
            P(("dp", "fsdp")),
            P(("dp", "fsdp")),
            P(("dp", "fsdp"), None),
            P(("dp", "fsdp")),
            P(("dp", "fsdp"), None),
            P(("dp", "fsdp")),
            P(("dp", "fsdp")),
            P(("dp", "fsdp")),
        ),
        check_vma=False,
    )
```
